256 devices in a mesh: ta: 4 (over y), gz: 4 (over x_hi, core), xy: 16 (over x_lo, z).
Axes of the slice: x: 4 (x_hi: 2, x_lo: 2; x = x_hi * 2 + x_lo), y: 4, z: 8, core: 2. Of those that a mesh axis runs over, the one named last changes fastest.
Arguments:
- links: float32 [4, 2, 3, 3, 4, 64, 512], P(None, None, None, None, 'ta', 'xy', 'gz'), may hold values from -0.72 to 1.72
- guess: float32 [12, 2, 4, 3, 4, 64, 512], P(None, None, None, None, 'ta', 'xy', 'gz'), may hold values from -1.5 to 1.5
- source_sites: int32 [4, 16, 4, 4], P('ta', 'xy', 'gz'), may hold values from 0 to 31, as said below
Outputs:
- solution: float32 [12, 2, 4, 3, 4, 64, 512], P(None, None, None, None, 'ta', 'xy', 'gz')
- residual: float32 [12, 2, 4, 3, 4, 64, 512], P(None, None, None, None, 'ta', 'xy', 'gz')
The draws below stay inside these ranges and needn't reach their ends.
Inputs may be any that keep to these rules, and one draw needn't show every extreme that they name: `source_sites`: each entry is an offset inside its block: time below 1, y below 4, z below 4, x below 32.
All inputs are finite; a program needn't handle non-finite values.
Results may differ from the reference program's by a relative error of at most 0.00012.
Values sent between devices are 32-bit elements; how exact they have to be, the bound alone decides.
No kernel may reach another device: no remote copies, remote signals or barrier semaphores. Data moves between devices by JAX's collectives and lax.ppermute only.
A program may use at most 128 MiB of HBM per device.

```python
import math
import jax
import jax.numpy as jnp
import numpy as np
from jax import lax

LT = 1
LY = 4
LZ = 4
LX = 32
NSMEAR = 8
NT = 4
NY = 64
NZ = 16


def draw_links(key, part):
    full_shape = (4, 2, 3, 3, NT, NY, NZ * LX)
    noise = 0.18 * jnp.clip(jax.random.normal(key, full_shape), -4.0, 4.0)
    identity = jnp.eye(3, dtype=jnp.float32)
    unit = jnp.stack([identity, jnp.zeros_like(identity)], axis=0)
    return (unit[None, :, :, :, None, None, None] + noise).astype(jnp.float32)


def draw_guess(key, part):
    main_key, slice_key = jax.random.split(key)
    full_shape = (12, 2, 4, 3, NT, NY, NZ * LX)
    rising = 10.0 ** (jnp.arange(NT, dtype=jnp.float32) / NT)
    slices = jax.random.uniform(slice_key, (NZ,), minval=0.0, maxval=math.log(3.0))
    slice_scale = jnp.repeat(jnp.exp(slices), LX)
    noise = jnp.clip(jax.random.normal(main_key, full_shape), -5.0, 5.0)
    return (0.01 * noise * rising[:, None, None] * slice_scale).astype(jnp.float32)


def draw_source_sites(key, part):
    blocks = (NT // LT, NY // LY, NZ // LZ)
    subkeys = jax.random.split(key, 4)
    limits = (LT, LY, LZ, LX)
    columns = [jax.random.randint(subkeys[position], blocks, 0, limits[position]) for position in range(4)]
    return jnp.stack(columns, axis=-1).astype(jnp.int32)


def setup_inputs(seed: int = 0) -> dict:
    arg_keys = jax.random.split(jax.random.key(seed), 4)
    links = draw_links(jax.random.fold_in(arg_keys[3], 71), 0)
    guess = draw_guess(jax.random.fold_in(arg_keys[3], 71), 0)
    source_sites = draw_source_sites(jax.random.fold_in(arg_keys[3], 71), 0)
    return dict(links=links, guess=guess, source_sites=source_sites)


HIGHEST = lax.Precision.HIGHEST
hopping = 0.12
smear_weight = 0.25
smear_norm = 2.0


def pauli_blocks():
    sigma_one = np.array([[0, 1], [1, 0]], dtype=complex)
    sigma_two = np.array([[0, -1j], [1j, 0]], dtype=complex)
    sigma_three = np.array([[1, 0], [0, -1]], dtype=complex)
    return [-1j * sigma_one, -1j * sigma_two, -1j * sigma_three, np.eye(2, dtype=complex)]


def real_form(matrix):
    upper = np.concatenate([matrix.real, -matrix.imag], axis=1)
    lower = np.concatenate([matrix.imag, matrix.real], axis=1)
    return np.concatenate([upper, lower], axis=0).astype(np.float32)


def full_table(direction, parity):
    block_matrix = pauli_blocks()[direction]
    project_rows = np.concatenate([np.eye(2), parity * block_matrix], axis=1)
    lift_rows = np.concatenate([np.eye(2), parity * block_matrix.conj().T], axis=0)
    return real_form(lift_rows @ project_rows)


def spin_apply(matrix, field):
    spin_table = jnp.asarray(matrix)
    copies = field.shape[0]
    flattened = field.reshape((copies, spin_table.shape[1]) + field.shape[3:])
    applied = jnp.einsum('ij,rjatyw->riatyw', spin_table, flattened, precision=HIGHEST)
    return applied.reshape((copies, 2, spin_table.shape[0] // 2) + field.shape[3:])


def colour_times(link, field, adjoint):
    form = 'batyw,...btyw->...atyw' if adjoint else 'abtyw,...btyw->...atyw'
    parity = -1.0 if adjoint else 1.0
    real_part = field[:, 0]
    imag_part = field[:, 1]
    out_real = jnp.einsum(form, link[0], real_part, precision=HIGHEST) - parity * jnp.einsum(form, link[1], imag_part, precision=HIGHEST)
    out_imag = jnp.einsum(form, link[0], imag_part, precision=HIGHEST) + parity * jnp.einsum(form, link[1], real_part, precision=HIGHEST)
    return jnp.stack([out_real, out_imag], axis=1)


def roll_x(field, amount):
    shaped = field.reshape(field.shape[:-1] + (field.shape[-1] // LX, LX))
    return jnp.roll(shaped, amount, axis=-1).reshape(field.shape)


def shift_ahead(field, direction):
    if direction == 0:
        return roll_x(field, -1)
    if direction == 1:
        return jnp.roll(field, -1, axis=-2)
    if direction == 2:
        return jnp.roll(field, -LX, axis=-1)
    return jnp.roll(field, -1, axis=-3)


def shift_behind(field, direction):
    if direction == 0:
        return roll_x(field, 1)
    if direction == 1:
        return jnp.roll(field, 1, axis=-2)
    if direction == 2:
        return jnp.roll(field, LX, axis=-1)
    return jnp.roll(field, 1, axis=-3)


def point_sources(source_sites):
    time_ids = jnp.arange(NT, dtype=jnp.int32)
    row_ids = jnp.arange(NY, dtype=jnp.int32)
    slice_ids = jnp.arange(NZ, dtype=jnp.int32)
    column_ids = jnp.arange(LX, dtype=jnp.int32)
    offsets = source_sites[(time_ids // LT)[:, None, None], (row_ids // LY)[None, :, None], (slice_ids // LZ)[None, None, :]]
    site_hit = (offsets[..., 0] == (time_ids % LT)[:, None, None]) & (offsets[..., 1] == (row_ids % LY)[None, :, None]) & (offsets[..., 2] == (slice_ids % LZ)[None, None, :])
    site_hit = site_hit[..., None] & (offsets[..., 3:4] == column_ids)
    mask = jnp.where(site_hit, 1.0, 0.0).astype(jnp.float32).reshape(NT, NY, NZ * LX)
    identity = jnp.eye(3, dtype=jnp.float32)
    real_part = identity[:, :, None, None, None] * mask
    return jnp.stack([real_part, jnp.zeros_like(real_part)], axis=1)


def smear_step(colour_field, links):
    total = jnp.zeros_like(colour_field)
    for direction in range(3):
        link = links[direction]
        ahead_part = colour_times(link, shift_ahead(colour_field, direction), False)
        behind_part = shift_behind(colour_times(link, colour_field, True), direction)
        total = total + ahead_part + behind_part
    return (colour_field + smear_weight * total) / smear_norm


def spread(colour_field):
    identity = jnp.eye(4, dtype=jnp.float32)
    grown = identity[:, None, None, :, None, None, None, None] * colour_field[None, :, :, None, :, :, :, :]
    return grown.reshape((12, 2, 4, 3) + colour_field.shape[3:])


def wilson_single(field, links):
    time_ids = jnp.arange(NT, dtype=jnp.int32)
    ahead_parity = jnp.where(time_ids == NT - 1, -1.0, 1.0).astype(jnp.float32)[:, None, None]
    behind_parity = jnp.where(time_ids == 0, -1.0, 1.0).astype(jnp.float32)[:, None, None]
    total = jnp.zeros_like(field)
    for direction in range(4):
        link = links[direction]
        ahead_part = shift_ahead(field, direction)
        behind_part = shift_behind(colour_times(link, field, True), direction)
        if direction == 3:
            ahead_part = ahead_part * ahead_parity
            behind_part = behind_part * behind_parity
        ahead_part = colour_times(link, ahead_part, False)
        total = total + spin_apply(full_table(direction, -1.0), ahead_part) + spin_apply(full_table(direction, 1.0), behind_part)
    return field - hopping * total


def wilson(field, links):
    return lax.map(lambda single: wilson_single(single[None], links)[0], field)


def dagger(field, links):
    chirality = jnp.array([1.0, 1.0, -1.0, -1.0], dtype=jnp.float32)[None, None, :, None, None, None, None]
    return chirality * wilson(chirality * field, links)


def reference(links, guess, source_sites):
    colour_field = point_sources(source_sites)
    for iteration in range(NSMEAR):
        colour_field = smear_step(colour_field, links)
    right_side = spread(colour_field)
    defect = right_side - wilson(guess, links)
    search = dagger(defect, links)
    applied = wilson(search, links)
    summed_axes = (1, 2, 3, 4, 5, 6)
    norm_now = jnp.sum(search * search, axis=summed_axes)
    curvature = jnp.sum(applied * applied, axis=summed_axes)
    step_length = (norm_now / curvature)[:, None, None, None, None, None, None]
    solution = guess + step_length * search
    residual = search - step_length * dagger(applied, links)
    return solution, residual
```

```python
import jax
import jax.numpy as jnp
import numpy as np
from jax import lax
from jax.experimental import pallas as pl
from jax.experimental.pallas import tpu as pltpu
from jax.sharding import PartitionSpec as P

LX = 32
HOPPING = 0.12
PAIRS = 6


def pauli_blocks():
    sigma_one = np.array([[0, 1], [1, 0]], dtype=complex)
    sigma_two = np.array([[0, -1j], [1j, 0]], dtype=complex)
    sigma_three = np.array([[1, 0], [0, -1]], dtype=complex)
    return [-1j * sigma_one, -1j * sigma_two, -1j * sigma_three, np.eye(2, dtype=complex)]


E_BLOCKS = pauli_blocks()


def roll(value, shift, axis):
    size = value.shape[axis]
    shift = shift % size
    return value if shift == 0 else pltpu.roll(value, shift, axis)


def rows():
    return lax.broadcasted_iota(jnp.int32, (8, 128), 0)


def lanes():
    return lax.broadcasted_iota(jnp.int32, (8, 128), 1)


def add_phase(base, phase, value):
    real, imag = value
    if phase == 1:
        return (base[0] + real, base[1] + imag)
    if phase == -1:
        return (base[0] - real, base[1] - imag)
    if phase == 1j:
        return (base[0] - imag, base[1] + real)
    return (base[0] + imag, base[1] - real)


def load_field(ref, pair):
    base = pair * 24
    return [
        [(ref[base + s * 3 + c], ref[base + 12 + s * 3 + c]) for c in range(3)] for s in range(4)
    ]


def project(field, mu, parity):
    block = E_BLOCKS[mu]
    half = []
    for a in range(2):
        b = int(np.flatnonzero(np.abs(block[a]) > 0.5)[0])
        phase = complex(parity * block[a, b])
        half.append([add_phase(field[a][c], phase, field[2 + b][c]) for c in range(3)])
    return half


def lift(total, half, mu, parity):
    block = E_BLOCKS[mu]
    for a in range(2):
        b = int(np.flatnonzero(np.abs(block[a]) > 0.5)[0])
        phase = complex(parity * np.conj(block[a, b]))
        for c in range(3):
            total[a][c] = add_phase(total[a][c], 1, half[a][c])
            total[2 + b][c] = add_phase(total[2 + b][c], phase, half[a][c])


def load_link(ref, base, stride, mu):
    return [
        [
            (
                ref[base + stride * (mu * 18 + a * 3 + b)],
                ref[base + stride * (mu * 18 + 9 + a * 3 + b)],
            )
            for b in range(3)
        ]
        for a in range(3)
    ]


def times(link, vector):
    out = []
    for a in range(3):
        real = imag = None
        for b in range(3):
            ur, ui = link[a][b]
            vr, vi = vector[b]
            tr = ur * vr - ui * vi
            ti = ur * vi + ui * vr
            real = tr if real is None else real + tr
            imag = ti if imag is None else imag + ti
        out.append((real, imag))
    return out


def times_adjoint(link, vector):
    out = []
    for a in range(3):
        real = imag = None
        for b in range(3):
            ur, ui = link[b][a]
            vr, vi = vector[b]
            tr = ur * vr + ui * vi
            ti = ur * vi - ui * vr
            real = tr if real is None else real + tr
            imag = ti if imag is None else imag + ti
        out.append((real, imag))
    return out


def flat(half):
    return [half[a][c][part] for part in range(2) for a in range(2) for c in range(3)]


def unflat(values):
    return [[(values[a * 3 + c], values[6 + a * 3 + c]) for c in range(3)] for a in range(2)]


def map_half(half, fn):
    return [[(fn(re), fn(im)) for re, im in spin] for spin in half]


def pick4(index, parts):
    return jnp.where(
        index < 2,
        jnp.where(index == 0, parts[0], parts[1]),
        jnp.where(index == 2, parts[2], parts[3]),
    )


def x_ahead(value):
    return jnp.where(lanes() % LX == LX - 1, roll(value, LX - 1, 1), roll(value, -1, 1))


def x_behind(value):
    return jnp.where(lanes() % LX == 0, roll(value, 1 - LX, 1), roll(value, 1, 1))


def make_sends(field, pair, links, sign, outs):
    t_ahead, t_behind, y_ahead, y_behind, z_ahead, z_behind, carried_y, carried_z = outs
    row4 = rows() % 4
    group = lanes() // LX
    half = flat(project(field, 3, -sign))
    for i in range(12):
        t_ahead[pair * 12 + i] = half[i]
    link = load_link(links, 0, 1, 3)
    half = flat([times_adjoint(link, v) for v in project(field, 3, sign)])
    for i in range(12):
        t_behind[pair * 12 + i] = half[i]
    half = flat(project(field, 1, -sign))
    for q in range(3):
        y_ahead[pair * 3 + q] = pick4(row4, [roll(half[4 * q + j], j, 0) for j in range(4)])
    link = load_link(links, 0, 1, 1)
    half = flat([times_adjoint(link, v) for v in project(field, 1, sign)])
    for i in range(12):
        carried_y[pair * 12 + i] = half[i]
    for q in range(3):
        y_behind[pair * 3 + q] = pick4(row4, [roll(half[4 * q + j], j - 3, 0) for j in range(4)])
    half = flat(project(field, 2, -sign))
    for q in range(3):
        z_ahead[pair * 3 + q] = pick4(group, [roll(half[4 * q + j], LX * j, 1) for j in range(4)])
    link = load_link(links, 0, 1, 2)
    half = flat([times_adjoint(link, v) for v in project(field, 2, sign)])
    for i in range(12):
        carried_z[pair * 12 + i] = half[i]
    for q in range(3):
        z_behind[pair * 3 + q] = pick4(
            group, [roll(half[4 * q + j], LX * (j - 3), 1) for j in range(4)]
        )


def apply_wilson(field, pair, links, sign, halos, carried_y, carried_z):
    t_ahead, t_behind, y_ahead, y_behind, z_ahead, z_behind = halos
    row4 = rows() % 4
    group = lanes() // LX
    zero = jnp.zeros((8, 128), jnp.float32)
    total = [[(zero, zero) for _ in range(3)] for _ in range(4)]
    link = load_link(links, 0, 1, 0)
    half = map_half(project(field, 0, -sign), x_ahead)
    lift(total, [times(link, v) for v in half], 0, -sign)
    half = [times_adjoint(link, v) for v in project(field, 0, sign)]
    lift(total, map_half(half, x_behind), 0, sign)
    link = load_link(links, 0, 1, 1)
    half = flat(project(field, 1, -sign))
    packed = [y_ahead[pair * 3 + q] for q in range(3)]
    half = [
        jnp.where(row4 == 3, roll(packed[i // 4], 3 - i % 4, 0), roll(half[i], -1, 0))
        for i in range(12)
    ]
    lift(total, [times(link, v) for v in unflat(half)], 1, -sign)
    packed = [y_behind[pair * 3 + q] for q in range(3)]
    half = [
        jnp.where(
            row4 == 0, roll(packed[i // 4], -(i % 4), 0), roll(carried_y[pair * 12 + i], 1, 0)
        )
        for i in range(12)
    ]
    lift(total, unflat(half), 1, sign)
    link = load_link(links, 0, 1, 2)
    half = flat(project(field, 2, -sign))
    packed = [z_ahead[pair * 3 + q] for q in range(3)]
    half = [
        jnp.where(group == 3, roll(packed[i // 4], LX * (3 - i % 4), 1), roll(half[i], -LX, 1))
        for i in range(12)
    ]
    lift(total, [times(link, v) for v in unflat(half)], 2, -sign)
    packed = [z_behind[pair * 3 + q] for q in range(3)]
    half = [
        jnp.where(
            group == 0,
            roll(packed[i // 4], -LX * (i % 4), 1),
            roll(carried_z[pair * 12 + i], LX, 1),
        )
        for i in range(12)
    ]
    lift(total, unflat(half), 2, sign)
    link = load_link(links, 0, 1, 3)
    half = unflat([t_ahead[pair * 12 + i] for i in range(12)])
    lift(total, [times(link, v) for v in half], 3, -sign)
    half = unflat([t_behind[pair * 12 + i] for i in range(12)])
    lift(total, half, 3, sign)
    return [
        [
            tuple(field[s][c][k] - HOPPING * total[s][c][k] for k in range(2))
            for c in range(3)
        ]
        for s in range(4)
    ]


def store_field(ref, pair, field):
    for s in range(4):
        for c in range(3):
            ref[pair * 24 + s * 3 + c] = field[s][c][0]
            ref[pair * 24 + 12 + s * 3 + c] = field[s][c][1]


def norm_row(partials, offset):
    row = rows()
    lane = lanes()
    total = jnp.zeros((8, 128), jnp.float32)
    for pair in range(PAIRS):
        sums = jnp.sum(partials[pair], axis=1, keepdims=True)
        keep = lane == offset + 2 * pair + row // 4
        total = total + jnp.where(keep, sums, 0.0)
    return jnp.sum(total, axis=0, keepdims=True)


def squares(field):
    total = None
    for s in range(4):
        for c in range(3):
            for k in range(2):
                term = field[s][c][k] * field[s][c][k]
                total = term if total is None else total + term
    return total


def block_kernel(sites, links, out):
    for k in range(27):
        out[8 * k : 8 * k + 8] = links[8 * k : 8 * k + 8]
    hit = (rows() == sites[1]) & (lanes() == sites[2] * LX + sites[3]) & (sites[0] == 0)
    out[216:224] = jnp.where(hit, 1.0, 0.0).astype(jnp.float32)


def prepare_kernel(last_time, guess, links, field, pair_links, *sends):
    low = rows() < 4
    for k in range(36):
        value = links[8 * k : 8 * k + 8]
        if k >= 27:
            crossing = lax.axis_index("ta") == last_time
            value = jnp.where(crossing, -value, value)
        other = roll(value, 4, 0)
        pair_links[2 * k] = jnp.where(low, value, other)
        pair_links[2 * k + 1] = jnp.where(low, other, value)

    def body(pair, carry):
        for k in range(12):
            start = pl.multiple_of(pair * 192 + 8 * k, 8)
            first = guess[pl.ds(start, 8)]
            second = guess[pl.ds(start + 96, 8)]
            field[pair * 24 + 2 * k] = jnp.where(low, first, roll(second, 4, 0))
            field[pair * 24 + 2 * k + 1] = jnp.where(low, roll(first, 4, 0), second)
        make_sends(load_field(field, pair), pair, pair_links, 1.0, sends)
        return carry

    lax.fori_loop(0, PAIRS, body, 0)


def first_kernel(field, links, ta, tb, ya, yb, za, zb, cy, cz, out):
    def body(pair, carry):
        value = apply_wilson(
            load_field(field, pair), pair, links, 1.0, (ta, tb, ya, yb, za, zb), cy, cz
        )
        store_field(out, pair, value)
        return carry

    lax.fori_loop(0, PAIRS, body, 0)


def defect_kernel(applied, smeared, links, out, *sends):
    low = rows() < 4
    for pair in range(PAIRS):
        spins = [(2 * pair + h) // 3 for h in range(2)]
        colours = [(2 * pair + h) % 3 for h in range(2)]
        for part in range(2):
            for s in range(4):
                for a in range(3):
                    index = pair * 24 + part * 12 + s * 3 + a
                    source = [
                        smeared[colours[h] * 6 + part * 3 + a] if spins[h] == s else 0.0
                        for h in range(2)
                    ]
                    if s in spins:
                        out[index] = jnp.where(low, source[0], source[1]) - applied[index]
                    else:
                        out[index] = -applied[index]

    def body(pair, carry):
        make_sends(load_field(out, pair), pair, links, -1.0, sends)
        return carry

    lax.fori_loop(0, PAIRS, body, 0)


def search_kernel(field, links, ta, tb, ya, yb, za, zb, cy, cz, out, norm, *rest):
    sends, partials = rest[:8], rest[8]

    def body(pair, carry):
        value = apply_wilson(
            load_field(field, pair), pair, links, -1.0, (ta, tb, ya, yb, za, zb), cy, cz
        )
        store_field(out, pair, value)
        partials[pair] = squares(value)
        make_sends(load_field(out, pair), pair, links, 1.0, sends)
        return carry

    lax.fori_loop(0, PAIRS, body, 0)
    norm[...] = jnp.broadcast_to(norm_row([partials[p] for p in range(PAIRS)], 0), (8, 128))


def applied_kernel(field, links, ta, tb, ya, yb, za, zb, cy, cz, norm, out, sums, *rest):
    sends, partials = rest[:8], rest[8]

    def body(pair, carry):
        value = apply_wilson(
            load_field(field, pair), pair, links, 1.0, (ta, tb, ya, yb, za, zb), cy, cz
        )
        store_field(out, pair, value)
        partials[pair] = squares(value)
        make_sends(load_field(out, pair), pair, links, -1.0, sends)
        return carry

    lax.fori_loop(0, PAIRS, body, 0)
    row = norm_row([partials[p] for p in range(PAIRS)], 16)
    both = norm[...] + jnp.broadcast_to(row, (8, 128))
    for k in range(sums.shape[0] // 8):
        sums[8 * k : 8 * k + 8] = both


def final_kernel(applied, links, ta, tb, ya, yb, za, zb, cy, cz, sums, guess, search, solution, residual, steps):
    low = rows() < 4
    lane = lanes()
    parts = [sums[8 * k : 8 * k + 8] for k in range(sums.shape[0] // 8)]
    while len(parts) > 1:
        odd = parts[-1:] if len(parts) % 2 else []
        parts = [a + b for a, b in zip(parts[::2], parts[1::2])] + odd
    total = jnp.broadcast_to(jnp.sum(parts[0], axis=0, keepdims=True), (8, 128))
    curvature = jnp.where(lane < 12, roll(total, -16, 1), 1.0)
    ratio = total / curvature
    for pair in range(PAIRS):
        keep = lane == 2 * pair + rows() // 4
        step = jnp.sum(jnp.where(keep, ratio, 0.0), axis=1, keepdims=True)
        steps[pair] = jnp.broadcast_to(step, (8, 128))

    def body(pair, carry):
        value = apply_wilson(
            load_field(applied, pair), pair, links, -1.0, (ta, tb, ya, yb, za, zb), cy, cz
        )
        step = steps[pair]
        direction = load_field(search, pair)
        residue = [None] * 24
        update = [None] * 24
        for s in range(4):
            for c in range(3):
                for k in range(2):
                    index = k * 12 + s * 3 + c
                    residue[index] = direction[s][c][k] - step * value[s][c][k]
                    update[index] = step * direction[s][c][k]
        for k in range(12):
            start = pl.multiple_of(pair * 192 + 8 * k, 8)
            even, odd = residue[2 * k], residue[2 * k + 1]
            residual[pl.ds(start, 8)] = jnp.where(low, even, roll(odd, 4, 0))
            residual[pl.ds(start + 96, 8)] = jnp.where(low, roll(even, 4, 0), odd)
            even, odd = update[2 * k], update[2 * k + 1]
            solution[pl.ds(start, 8)] = guess[pl.ds(start, 8)] + jnp.where(
                low, even, roll(odd, 4, 0)
            )
            solution[pl.ds(start + 96, 8)] = guess[pl.ds(start + 96, 8)] + jnp.where(
                low, roll(even, 4, 0), odd
            )
        return carry

    lax.fori_loop(0, PAIRS, body, 0)


def gather_rows(own, below, above):
    row = rows()
    inside = (row >= 2) & (row < 6)
    out = []
    for odd in range(2):
        shift = 6 if odd else 2
        o = roll(own, shift, 0)
        lo = roll(below, 8 - shift, 0)
        hi = roll(above, 8 - shift, 0)
        tile_a = jnp.where(inside, o, jnp.where(row < 2, lo, hi))
        tile_b = jnp.where(row < 4, hi, lo)
        out.append((tile_a, tile_b))
    return out


def colour_field(ref, base, colour):
    return [(ref[base + colour * 6 + a], ref[base + colour * 6 + 3 + a]) for a in range(3)]


def store_colour(ref, base, colour, value):
    for a in range(3):
        ref[base + colour * 6 + a] = value[a][0]
        ref[base + colour * 6 + 3 + a] = value[a][1]


def map_colour(value, fn):
    return [(fn(re), fn(im)) for re, im in value]


def zip_colour(first, second, fn):
    return [(fn(a[0], b[0]), fn(a[1], b[1])) for a, b in zip(first, second)]


def smear_iteration(links_a, links_b, src_a, src_b, dst_a, dst_b, carried_a, carried_b, use_b, make_b):
    def carry_z(column, carry):
        base = column * 54
        for links, src, carried, wanted in (
            (links_a, src_a, carried_a, True),
            (links_b, src_b, carried_b, make_b),
        ):
            if wanted:
                link = load_link(links, base, 1, 2)
                for colour in range(3):
                    value = times_adjoint(link, colour_field(src, column * 18, colour))
                    store_colour(carried, column * 18, colour, value)
        return carry

    lax.fori_loop(0, 4, carry_z, 0)
    row = rows()
    lane = lanes()

    def update(column, carry):
        base = column * 54
        here = column * 18
        ahead_column = ((column + 1) & 3) * 18
        behind_column = ((column + 3) & 3) * 18

        def z_part(links, src, carried, colour):
            link = load_link(links, base, 1, 2)
            ahead = zip_colour(
                colour_field(src, here, colour),
                colour_field(src, ahead_column, colour),
                lambda a, b: jnp.where(lane < 96, roll(a, -LX, 1), roll(b, -LX, 1)),
            )
            behind = zip_colour(
                colour_field(carried, here, colour),
                colour_field(carried, behind_column, colour),
                lambda a, b: jnp.where(lane >= LX, roll(a, LX, 1), roll(b, LX, 1)),
            )
            return zip_colour(times(link, ahead), behind, lambda a, b: a + b)

        def x_part(links, src, colour):
            link = load_link(links, base, 1, 0)
            value = colour_field(src, here, colour)
            ahead = times(link, map_colour(value, x_ahead))
            behind = map_colour(times_adjoint(link, value), x_behind)
            return zip_colour(ahead, behind, lambda a, b: a + b)

        def y_parts(colour):
            link_a = load_link(links_a, base, 1, 1)
            value_a = colour_field(src_a, here, colour)
            product_a = times_adjoint(link_a, value_a)
            if not use_b:
                ahead_a = times(link_a, map_colour(value_a, lambda v: roll(v, -1, 0)))
                behind_a = map_colour(product_a, lambda v: roll(v, 1, 0))
                return zip_colour(ahead_a, behind_a, lambda a, b: a + b), None
            link_b = load_link(links_b, base, 1, 1)
            value_b = colour_field(src_b, here, colour)
            product_b = times_adjoint(link_b, value_b)

            def ahead_of(first, second):
                return zip_colour(
                    first,
                    second,
                    lambda a, b: jnp.where(row == 7, roll(b, -1, 0), roll(a, -1, 0)),
                )

            def behind_of(first, second):
                return zip_colour(
                    first, second, lambda a, b: jnp.where(row == 0, roll(b, 1, 0), roll(a, 1, 0))
                )

            part_a = zip_colour(
                times(link_a, ahead_of(value_a, value_b)),
                behind_of(product_a, product_b),
                lambda a, b: a + b,
            )
            if not make_b:
                return part_a, None
            part_b = zip_colour(
                times(link_b, ahead_of(value_b, value_a)),
                behind_of(product_b, product_a),
                lambda a, b: a + b,
            )
            return part_a, part_b

        for colour in range(3):
            y_a, y_b = y_parts(colour)
            jobs = [(links_a, src_a, carried_a, dst_a, y_a)]
            if make_b:
                jobs.append((links_b, src_b, carried_b, dst_b, y_b))
            for links, src, carried, dst, y_part in jobs:
                total = zip_colour(x_part(links, src, colour), y_part, lambda a, b: a + b)
                total = zip_colour(total, z_part(links, src, carried, colour), lambda a, b: a + b)
                value = zip_colour(
                    colour_field(src, here, colour), total, lambda a, b: (a + 0.25 * b) * 0.5
                )
                store_colour(dst, here, colour, value)
        return carry

    lax.fori_loop(0, 4, update, 0)


def four_iterations(links_a, links_b, fa, fb, ga, gb, carried_a, carried_b):
    common = (carried_a, carried_b)
    smear_iteration(links_a, links_b, fa, fb, ga, gb, *common, True, True)
    smear_iteration(links_a, links_b, ga, gb, fa, fb, *common, True, False)
    smear_iteration(links_a, links_b, fa, fb, ga, gb, *common, False, False)
    smear_iteration(links_a, links_b, ga, gb, fa, fb, *common, False, False)


def smear_first_kernel(own, below, above, links_a, links_b, out, fa, fb, ga, gb, ca, cb):
    low = rows() < 4

    def build(column, carry):
        base = column * 224
        for k in range(28):
            start = pl.multiple_of(base + 8 * k, 8)
            tiles = gather_rows(
                own[pl.ds(start, 8)], below[pl.ds(start, 8)], above[pl.ds(start, 8)]
            )
            if k < 27:
                for odd in range(2):
                    links_a[column * 54 + 2 * k + odd] = tiles[odd][0]
                    links_b[column * 54 + 2 * k + odd] = tiles[odd][1]
        mask_a, mask_b = tiles[0]
        zero = jnp.zeros((8, 128), jnp.float32)
        for colour in range(3):
            for part in range(2):
                for a in range(3):
                    index = column * 18 + colour * 6 + part * 3 + a
                    is_point = part == 0 and a == colour
                    fa[index] = mask_a if is_point else zero
                    fb[index] = mask_b if is_point else zero
        return carry

    lax.fori_loop(0, 4, build, 0)
    four_iterations(links_a, links_b, fa, fb, ga, gb, ca, cb)

    def pack(column, carry):
        for k in range(9):
            even = roll(fa[column * 18 + 2 * k], 6, 0)
            odd = roll(fa[column * 18 + 2 * k + 1], 2, 0)
            out[column * 9 + k] = jnp.where(low, even, odd)
        return carry

    lax.fori_loop(0, 4, pack, 0)


def smear_second_kernel(links_a, links_b, own, below, above, out, fa, fb, ga, gb, ca, cb):
    low = rows() < 4

    def build(column, carry):
        for k in range(9):
            index = column * 9 + k
            tiles = gather_rows(own[index], below[index], above[index])
            for odd in range(2):
                fa[column * 18 + 2 * k + odd] = tiles[odd][0]
                fb[column * 18 + 2 * k + odd] = tiles[odd][1]
        return carry

    lax.fori_loop(0, 4, build, 0)
    four_iterations(links_a, links_b, fa, fb, ga, gb, ca, cb)
    for i in range(18):
        out[i] = jnp.where(low, roll(fa[i], 6, 0), roll(fa[i], 2, 0))


def call(kernel, name, outs, args, scratch=(), flops=0, scalars=0):
    vmem = pl.BlockSpec(memory_space=pltpu.VMEM)
    smem = pl.BlockSpec(memory_space=pltpu.SMEM)
    return pl.pallas_call(
        kernel,
        name=name,
        out_shape=[jax.ShapeDtypeStruct(shape, jnp.float32) for shape in outs],
        in_specs=[smem] * scalars + [vmem] * (len(args) - scalars),
        out_specs=[vmem] * len(outs),
        scratch_shapes=[pltpu.VMEM(shape, jnp.float32) for shape in scratch],
        compiler_params=pltpu.CompilerParams(vmem_limit_bytes=12 << 20),
        cost_estimate=pl.CostEstimate(flops=flops, bytes_accessed=0, transcendentals=0),
    )(*args)


def shift(value, axis, amount):
    n = lax.axis_size(axis)
    return lax.ppermute(value, axis, [(i, (i + amount) % n) for i in range(n)])


FULL = (144, 8, 128)
HALF = (72, 8, 128)
RIM = (18, 8, 128)
SENDS = [HALF, HALF, RIM, RIM, RIM, RIM, HALF, HALF]


def exchange(sends):
    ta, tb, ya, yb, za, zb, cy, cz = sends
    return (
        shift(ta, "ta", -1),
        shift(tb, "ta", 1),
        shift(ya, "xy", -1),
        shift(yb, "xy", 1),
        shift(za, "gz", -1),
        shift(zb, "gz", 1),
        cy,
        cz,
    )


def on_device(links, guess, source_sites):
    n_time = lax.axis_size("ta")
    axes = ("ta", "gz", "xy")
    devices = lax.axis_size(axes)
    link_rows = links.reshape(288, 128)
    guess_rows = guess.reshape(1152, 128)

    (block,) = call(
        block_kernel, "block", [(224, 128)], (source_sites.reshape(4), link_rows), scalars=1
    )
    columns = jnp.concatenate(
        [block, shift(block, "gz", -1), shift(block, "gz", -2), shift(block, "gz", 1)], axis=0
    )
    below, above = shift(columns, "xy", 1), shift(columns, "xy", -1)

    def prepare(*refs):
        prepare_kernel(n_time - 1, *refs)

    field, pair_links, *sends = call(
        prepare, "prepare", [FULL, HALF] + SENDS, (guess_rows, link_rows), flops=4000000
    )
    (applied,) = call(
        first_kernel, "wilson", [FULL], (field, pair_links, *exchange(sends)), flops=8000000
    )

    tiles = [(72, 8, 128)] * 6
    links_a, links_b, smeared = call(
        smear_first_kernel,
        "smear_first",
        [(216, 8, 128), (216, 8, 128), (36, 8, 128)],
        (columns, below, above),
        scratch=tiles,
        flops=30000000,
    )
    (smeared,) = call(
        smear_second_kernel,
        "smear_second",
        [(18, 8, 128)],
        (links_a, links_b, smeared, shift(smeared, "xy", 1), shift(smeared, "xy", -1)),
        scratch=tiles,
        flops=30000000,
    )
    defect, *sends = call(
        defect_kernel, "defect", [FULL] + SENDS, (applied, smeared, pair_links), flops=4000000
    )
    search, norm, *sends = call(
        search_kernel,
        "search",
        [FULL, (8, 128)] + SENDS,
        (defect, pair_links, *exchange(sends)),
        scratch=[(PAIRS, 8, 128)],
        flops=12000000,
    )
    applied, sums, *sends = call(
        applied_kernel,
        "applied",
        [FULL, (devices, 128)] + SENDS,
        (search, pair_links, *exchange(sends), norm),
        scratch=[(PAIRS, 8, 128)],
        flops=12000000,
    )
    halos = exchange(sends)
    sums = lax.all_to_all(sums, axes, 0, 0, tiled=True)
    solution, residual = call(
        final_kernel,
        "final",
        [(1152, 128), (1152, 128)],
        (applied, pair_links, *halos, sums, guess_rows, search),
        scratch=[(PAIRS, 8, 128)],
        flops=10000000,
    )
    return solution.reshape(guess.shape), residual.reshape(guess.shape)


def solution(mesh):
    spec = P(None, None, None, None, "ta", "xy", "gz")
    return jax.shard_map(
        on_device,
        mesh=mesh,
        in_specs=(spec, spec, P("ta", "xy", "gz", None)),
        out_specs=(spec, spec),
        check_vma=False,
    )
```

```python
import jax
import jax.numpy as jnp
import numpy as np
from jax import lax
from jax.experimental import pallas as pl
from jax.experimental.pallas import tpu as pltpu
from jax.sharding import Mesh
from jax.sharding import PartitionSpec as P

LX = 32
HOPPING = 0.12
PAIRS = 6
GZ = ("gh", "gc")


def pauli_blocks():
    sigma_one = np.array([[0, 1], [1, 0]], dtype=complex)
    sigma_two = np.array([[0, -1j], [1j, 0]], dtype=complex)
    sigma_three = np.array([[1, 0], [0, -1]], dtype=complex)
    return [-1j * sigma_one, -1j * sigma_two, -1j * sigma_three, np.eye(2, dtype=complex)]


E_BLOCKS = pauli_blocks()


def roll(value, shift, axis):
    size = value.shape[axis]
    shift = shift % size
    return value if shift == 0 else pltpu.roll(value, shift, axis)


def rows():
    return lax.broadcasted_iota(jnp.int32, (8, 128), 0)


def lanes():
    return lax.broadcasted_iota(jnp.int32, (8, 128), 1)


def add_phase(base, phase, value):
    real, imag = value
    if phase == 1:
        return (base[0] + real, base[1] + imag)
    if phase == -1:
        return (base[0] - real, base[1] - imag)
    if phase == 1j:
        return (base[0] - imag, base[1] + real)
    return (base[0] + imag, base[1] - real)


def load_field(ref, pair):
    base = pair * 24
    return [
        [(ref[base + s * 3 + c], ref[base + 12 + s * 3 + c]) for c in range(3)] for s in range(4)
    ]


def project(field, mu, parity):
    block = E_BLOCKS[mu]
    half = []
    for a in range(2):
        b = int(np.flatnonzero(np.abs(block[a]) > 0.5)[0])
        phase = complex(parity * block[a, b])
        half.append([add_phase(field[a][c], phase, field[2 + b][c]) for c in range(3)])
    return half


def lift(total, half, mu, parity):
    block = E_BLOCKS[mu]
    for a in range(2):
        b = int(np.flatnonzero(np.abs(block[a]) > 0.5)[0])
        phase = complex(parity * np.conj(block[a, b]))
        for c in range(3):
            total[a][c] = add_phase(total[a][c], 1, half[a][c])
            total[2 + b][c] = add_phase(total[2 + b][c], phase, half[a][c])


def load_link(ref, base, stride, mu):
    return [
        [
            (
                ref[base + stride * (mu * 18 + a * 3 + b)],
                ref[base + stride * (mu * 18 + 9 + a * 3 + b)],
            )
            for b in range(3)
        ]
        for a in range(3)
    ]


def times(link, vector):
    out = []
    for a in range(3):
        real = imag = None
        for b in range(3):
            ur, ui = link[a][b]
            vr, vi = vector[b]
            tr = ur * vr - ui * vi
            ti = ur * vi + ui * vr
            real = tr if real is None else real + tr
            imag = ti if imag is None else imag + ti
        out.append((real, imag))
    return out


def times_adjoint(link, vector):
    out = []
    for a in range(3):
        real = imag = None
        for b in range(3):
            ur, ui = link[b][a]
            vr, vi = vector[b]
            tr = ur * vr + ui * vi
            ti = ur * vi - ui * vr
            real = tr if real is None else real + tr
            imag = ti if imag is None else imag + ti
        out.append((real, imag))
    return out


def flat(half):
    return [half[a][c][part] for part in range(2) for a in range(2) for c in range(3)]


def unflat(values):
    return [[(values[a * 3 + c], values[6 + a * 3 + c]) for c in range(3)] for a in range(2)]


def map_half(half, fn):
    return [[(fn(re), fn(im)) for re, im in spin] for spin in half]


def pick4(index, parts):
    return jnp.where(
        index < 2,
        jnp.where(index == 0, parts[0], parts[1]),
        jnp.where(index == 2, parts[2], parts[3]),
    )


def x_ahead(value):
    return jnp.where(lanes() % LX == LX - 1, roll(value, LX - 1, 1), roll(value, -1, 1))


def x_behind(value):
    return jnp.where(lanes() % LX == 0, roll(value, 1 - LX, 1), roll(value, 1, 1))


def make_sends(field, pair, links, sign, outs):
    t_ahead, t_behind, y_ahead, y_behind, z_partner, z_other, *carried = outs
    even = lax.axis_index("gc") == 0
    row4 = rows() % 4
    group = lanes() // LX
    half = flat(project(field, 3, -sign))
    for i in range(12):
        t_ahead[pair * 12 + i] = half[i]
    link = load_link(links, 0, 1, 3)
    half = flat([times_adjoint(link, v) for v in project(field, 3, sign)])
    for i in range(12):
        t_behind[pair * 12 + i] = half[i]
    half = flat(project(field, 1, -sign))
    for q in range(3):
        y_ahead[pair * 3 + q] = pick4(row4, [roll(half[4 * q + j], j, 0) for j in range(4)])
    link = load_link(links, 0, 1, 1)
    half = flat([times_adjoint(link, v) for v in project(field, 1, sign)])
    for i in range(12 if carried else 0):
        carried[0][pair * 12 + i] = half[i]
    for q in range(3):
        y_behind[pair * 3 + q] = pick4(row4, [roll(half[4 * q + j], j - 3, 0) for j in range(4)])
    half = flat(project(field, 2, -sign))
    first = [pick4(group, [roll(half[4 * q + j], LX * j, 1) for j in range(4)]) for q in range(3)]
    link = load_link(links, 0, 1, 2)
    half = flat([times_adjoint(link, v) for v in project(field, 2, sign)])
    for i in range(12 if carried else 0):
        carried[1][pair * 12 + i] = half[i]
    for q in range(3):
        last = pick4(group, [roll(half[4 * q + j], LX * (j - 3), 1) for j in range(4)])
        z_partner[pair * 3 + q] = jnp.where(even, last, first[q])
        z_other[pair * 3 + q] = jnp.where(even, first[q], last)


def apply_wilson(field, pair, links, sign, halos, *carried):
    t_ahead, t_behind, y_ahead, y_behind, z_partner, z_other = halos
    even = lax.axis_index("gc") == 0
    row4 = rows() % 4
    group = lanes() // LX

    def carried_tiles(mu):
        if carried:
            return [carried[mu - 1][pair * 12 + i] for i in range(12)]
        return flat([times_adjoint(link, v) for v in project(field, mu, sign)])

    zero = jnp.zeros((8, 128), jnp.float32)
    total = [[(zero, zero) for _ in range(3)] for _ in range(4)]
    link = load_link(links, 0, 1, 0)
    half = map_half(project(field, 0, -sign), x_ahead)
    lift(total, [times(link, v) for v in half], 0, -sign)
    half = [times_adjoint(link, v) for v in project(field, 0, sign)]
    lift(total, map_half(half, x_behind), 0, sign)
    link = load_link(links, 0, 1, 1)
    half = flat(project(field, 1, -sign))
    packed = [y_ahead[pair * 3 + q] for q in range(3)]
    half = [
        jnp.where(row4 == 3, roll(packed[i // 4], 3 - i % 4, 0), roll(half[i], -1, 0))
        for i in range(12)
    ]
    lift(total, [times(link, v) for v in unflat(half)], 1, -sign)
    packed = [y_behind[pair * 3 + q] for q in range(3)]
    own = carried_tiles(1)
    half = [
        jnp.where(row4 == 0, roll(packed[i // 4], -(i % 4), 0), roll(own[i], 1, 0))
        for i in range(12)
    ]
    lift(total, unflat(half), 1, sign)
    link = load_link(links, 0, 1, 2)
    half = flat(project(field, 2, -sign))
    packed = [
        jnp.where(even, z_partner[pair * 3 + q], z_other[pair * 3 + q]) for q in range(3)
    ]
    half = [
        jnp.where(group == 3, roll(packed[i // 4], LX * (3 - i % 4), 1), roll(half[i], -LX, 1))
        for i in range(12)
    ]
    lift(total, [times(link, v) for v in unflat(half)], 2, -sign)
    packed = [
        jnp.where(even, z_other[pair * 3 + q], z_partner[pair * 3 + q]) for q in range(3)
    ]
    own = carried_tiles(2)
    half = [
        jnp.where(group == 0, roll(packed[i // 4], -LX * (i % 4), 1), roll(own[i], LX, 1))
        for i in range(12)
    ]
    lift(total, unflat(half), 2, sign)
    link = load_link(links, 0, 1, 3)
    half = unflat([t_ahead[pair * 12 + i] for i in range(12)])
    lift(total, [times(link, v) for v in half], 3, -sign)
    half = unflat([t_behind[pair * 12 + i] for i in range(12)])
    lift(total, half, 3, sign)
    return [
        [
            tuple(field[s][c][k] - HOPPING * total[s][c][k] for k in range(2))
            for c in range(3)
        ]
        for s in range(4)
    ]


def store_field(ref, pair, field):
    for s in range(4):
        for c in range(3):
            ref[pair * 24 + s * 3 + c] = field[s][c][0]
            ref[pair * 24 + 12 + s * 3 + c] = field[s][c][1]


def norm_row(partials, offset):
    row = rows()
    lane = lanes()
    total = jnp.zeros((8, 128), jnp.float32)
    for pair in range(PAIRS):
        sums = jnp.sum(partials[pair], axis=1, keepdims=True)
        keep = lane == offset + 2 * pair + row // 4
        total = total + jnp.where(keep, sums, 0.0)
    return jnp.sum(total, axis=0, keepdims=True)


def squares(field):
    total = None
    for s in range(4):
        for c in range(3):
            for k in range(2):
                term = field[s][c][k] * field[s][c][k]
                total = term if total is None else total + term
    return total


def block_kernel(source, links, out, sites, link_done, site_done):
    link_copy = pltpu.make_async_copy(links.at[0:216], out.at[0:216], link_done)
    site_copy = pltpu.make_async_copy(source, sites, site_done)
    link_copy.start()
    site_copy.start()
    site_copy.wait()
    hit = (rows() == sites[0, 1]) & (lanes() == sites[0, 2] * LX + sites[0, 3]) & (sites[0, 0] == 0)
    out[216:224] = jnp.where(hit, 1.0, 0.0).astype(jnp.float32)
    link_copy.wait()


def prepare_kernel(last_time, guess, links, field, pair_links, *sends):
    low = rows() < 4
    for k in range(36):
        value = links[8 * k : 8 * k + 8]
        if k >= 27:
            crossing = lax.axis_index("ta") == last_time
            value = jnp.where(crossing, -value, value)
        other = roll(value, 4, 0)
        pair_links[2 * k] = jnp.where(low, value, other)
        pair_links[2 * k + 1] = jnp.where(low, other, value)

    def body(pair, carry):
        for k in range(12):
            start = pl.multiple_of(pair * 192 + 8 * k, 8)
            first = guess[pl.ds(start, 8)]
            second = guess[pl.ds(start + 96, 8)]
            field[pair * 24 + 2 * k] = jnp.where(low, first, roll(second, 4, 0))
            field[pair * 24 + 2 * k + 1] = jnp.where(low, roll(first, 4, 0), second)
        make_sends(load_field(field, pair), pair, pair_links, 1.0, sends)
        return carry

    lax.fori_loop(0, PAIRS, body, 0)


def first_kernel(field, links, ta, tb, ya, yb, za, zb, cy, cz, out):
    def body(pair, carry):
        value = apply_wilson(
            load_field(field, pair), pair, links, 1.0, (ta, tb, ya, yb, za, zb), cy, cz
        )
        store_field(out, pair, value)
        return carry

    lax.fori_loop(0, PAIRS, body, 0)


def defect_kernel(applied, smeared, links, out, *sends):
    low = rows() < 4
    for pair in range(PAIRS):
        spins = [(2 * pair + h) // 3 for h in range(2)]
        colours = [(2 * pair + h) % 3 for h in range(2)]
        for part in range(2):
            for s in range(4):
                for a in range(3):
                    index = pair * 24 + part * 12 + s * 3 + a
                    source = [
                        smeared[colours[h] * 6 + part * 3 + a] if spins[h] == s else 0.0
                        for h in range(2)
                    ]
                    if s in spins:
                        out[index] = jnp.where(low, source[0], source[1]) - applied[index]
                    else:
                        out[index] = -applied[index]

    def body(pair, carry):
        make_sends(load_field(out, pair), pair, links, -1.0, sends)
        return carry

    lax.fori_loop(0, PAIRS, body, 0)


def search_kernel(field, links, ta, tb, ya, yb, za, zb, cy, cz, out, norm, *rest):
    sends, partials = rest[:8], rest[8]

    def body(pair, carry):
        value = apply_wilson(
            load_field(field, pair), pair, links, -1.0, (ta, tb, ya, yb, za, zb), cy, cz
        )
        store_field(out, pair, value)
        partials[pair] = squares(value)
        make_sends(load_field(out, pair), pair, links, 1.0, sends)
        return carry

    lax.fori_loop(0, PAIRS, body, 0)
    norm[...] = jnp.broadcast_to(norm_row([partials[p] for p in range(PAIRS)], 0), (8, 128))


def applied_kernel(field, links, ta, tb, ya, yb, za, zb, cy, cz, norm, out, sums, partials):
    def body(pair, carry):
        value = apply_wilson(
            load_field(field, pair), pair, links, 1.0, (ta, tb, ya, yb, za, zb), cy, cz
        )
        store_field(out, pair, value)
        partials[pair] = squares(value)
        return carry

    lax.fori_loop(0, PAIRS, body, 0)
    row = norm_row([partials[p] for p in range(PAIRS)], 16)
    sums[...] = norm[...] + jnp.broadcast_to(row, (8, 128))


def last_sends_kernel(field, links, *sends):
    def body(pair, carry):
        make_sends(load_field(field, pair), pair, links, -1.0, sends)
        return carry

    lax.fori_loop(0, PAIRS, body, 0)


def stencil_kernel(field, links, ta, tb, ya, yb, za, zb, out):
    def body(pair, carry):
        value = apply_wilson(
            load_field(field, pair), pair, links, -1.0, (ta, tb, ya, yb, za, zb)
        )
        store_field(out, pair, value)
        return carry

    lax.fori_loop(0, PAIRS, body, 0)


def column_sums(ref):
    parts = [ref[8 * k : 8 * k + 8] for k in range(ref.shape[0] // 8)]
    while len(parts) > 1:
        odd = parts[-1:] if len(parts) % 2 else []
        parts = [a + b for a, b in zip(parts[::2], parts[1::2])] + odd
    return jnp.broadcast_to(jnp.sum(parts[0], axis=0, keepdims=True), (8, 128))


def middle_kernel(own, partner, out):
    total = own[...] + partner[...]
    for k in range(out.shape[0] // 8):
        out[8 * k : 8 * k + 8] = total


def columns_kernel(own, far, out):
    out[0:224] = own[...]
    out[224:448] = far[...]


def final_kernel(normal, sums, guess, search, solution, residual, steps):
    low = rows() < 4
    lane = lanes()
    total = column_sums(sums)
    curvature = jnp.where(lane < 12, roll(total, -16, 1), 1.0)
    ratio = total / curvature
    for pair in range(PAIRS):
        keep = lane == 2 * pair + rows() // 4
        step = jnp.sum(jnp.where(keep, ratio, 0.0), axis=1, keepdims=True)
        steps[pair] = jnp.broadcast_to(step, (8, 128))

    def body(pair, carry):
        value = load_field(normal, pair)
        step = steps[pair]
        direction = load_field(search, pair)
        residue = [None] * 24
        update = [None] * 24
        for s in range(4):
            for c in range(3):
                for k in range(2):
                    index = k * 12 + s * 3 + c
                    residue[index] = direction[s][c][k] - step * value[s][c][k]
                    update[index] = step * direction[s][c][k]
        for k in range(12):
            start = pl.multiple_of(pair * 192 + 8 * k, 8)
            even, odd = residue[2 * k], residue[2 * k + 1]
            residual[pl.ds(start, 8)] = jnp.where(low, even, roll(odd, 4, 0))
            residual[pl.ds(start + 96, 8)] = jnp.where(low, roll(even, 4, 0), odd)
            even, odd = update[2 * k], update[2 * k + 1]
            solution[pl.ds(start, 8)] = guess[pl.ds(start, 8)] + jnp.where(
                low, even, roll(odd, 4, 0)
            )
            solution[pl.ds(start + 96, 8)] = guess[pl.ds(start + 96, 8)] + jnp.where(
                low, roll(even, 4, 0), odd
            )
        return carry

    lax.fori_loop(0, PAIRS, body, 0)


def gather_rows(own, below, above):
    row = rows()
    inside = (row >= 2) & (row < 6)
    out = []
    for odd in range(2):
        shift = 6 if odd else 2
        o = roll(own, shift, 0)
        lo = roll(below, 8 - shift, 0)
        hi = roll(above, 8 - shift, 0)
        tile_a = jnp.where(inside, o, jnp.where(row < 2, lo, hi))
        tile_b = jnp.where(row < 4, hi, lo)
        out.append((tile_a, tile_b))
    return out


def colour_field(ref, base, colour):
    return [(ref[base + colour * 6 + a], ref[base + colour * 6 + 3 + a]) for a in range(3)]


def store_colour(ref, base, colour, value):
    for a in range(3):
        ref[base + colour * 6 + a] = value[a][0]
        ref[base + colour * 6 + 3 + a] = value[a][1]


def map_colour(value, fn):
    return [(fn(re), fn(im)) for re, im in value]


def zip_colour(first, second, fn):
    return [(fn(a[0], b[0]), fn(a[1], b[1])) for a, b in zip(first, second)]


def nearest(i):
    return i + (i >> 1)


def four_columns(i):
    return i


def ahead_rows(first, second):
    return jnp.where(rows() == 7, roll(second, -1, 0), roll(first, -1, 0))


def behind_rows(first, second):
    return jnp.where(rows() == 0, roll(second, 1, 0), roll(first, 1, 0))


def ahead_columns(first, second):
    return jnp.where(lanes() < 96, roll(first, -LX, 1), roll(second, -LX, 1))


def behind_columns(first, second):
    return jnp.where(lanes() >= LX, roll(first, LX, 1), roll(second, LX, 1))


def add_colour(first, second):
    return zip_colour(first, second, lambda a, b: a + b)


def next_field(value, total):
    return zip_colour(value, total, lambda a, b: (a + 0.25 * b) * 0.5)


def point_iteration(links_a, links_b, mask_a, mask_b, dst_a, dst_b):
    def update(column, carry):
        base = column * 54
        behind_column = (column + 3) & 3
        ahead_column = (column + 1) & 3
        here_a, here_b = mask_a[column], mask_b[column]

        def conjugate(links, where, mu, colour, mask):
            link = load_link(links, where * 54, 1, mu)
            return [(link[colour][a][0] * mask, -link[colour][a][1] * mask) for a in range(3)]

        for links, dst, mask, other_mask, others in (
            (links_a, dst_a, here_a, here_b, links_b),
            (links_b, dst_b, here_b, here_a, links_a),
        ):
            masks = mask_a if dst is dst_a else mask_b
            shifted = [
                x_ahead(mask),
                ahead_rows(mask, other_mask),
                ahead_columns(mask, masks[ahead_column]),
            ]
            for colour in range(3):
                total = [
                    (shifted[0] * re, shifted[0] * im)
                    for re, im in (row[colour] for row in load_link(links, base, 1, 0))
                ]
                for mu in (1, 2):
                    link = load_link(links, base, 1, mu)
                    total = add_colour(
                        total,
                        [(shifted[mu] * r[colour][0], shifted[mu] * r[colour][1]) for r in link],
                    )
                product = conjugate(links, column, 0, colour, mask)
                total = add_colour(total, map_colour(product, x_behind))
                product = conjugate(links, column, 1, colour, mask)
                other = conjugate(others, column, 1, colour, other_mask)
                total = add_colour(total, zip_colour(product, other, behind_rows))
                product = conjugate(links, column, 2, colour, mask)
                other = conjugate(links, behind_column, 2, colour, masks[behind_column])
                total = add_colour(total, zip_colour(product, other, behind_columns))
                zero = jnp.zeros((8, 128), jnp.float32)
                value = [(mask if a == colour else zero, zero) for a in range(3)]
                store_colour(dst, column * 18, colour, next_field(value, total))
        return carry

    lax.fori_loop(0, 4, update, 0)


def smear_iteration(
    links_a, links_b, src_a, src_b, dst_a, dst_b, carried_a, carried_b, rims, carries, updates
):
    def carry_z(i, carry):
        column = carries[1](i)
        jobs = [(links_a, src_a, carried_a)] + [(links_b, src_b, carried_b)] * (rims == 2)
        for links, src, carried in jobs:
            link = load_link(links, column * 54, 1, 2)
            for colour in range(3):
                value = times_adjoint(link, colour_field(src, column * 18, colour))
                store_colour(carried, column * 18, colour, value)
        return carry

    lax.fori_loop(0, carries[0], carry_z, 0)

    def update(i, carry):
        column = updates[1](i)
        base = column * 54
        here = column * 18
        ahead_column = ((column + 1) & 3) * 18
        behind_column = ((column + 3) & 3) * 18

        def z_part(links, src, carried, colour):
            link = load_link(links, base, 1, 2)
            ahead = zip_colour(
                colour_field(src, here, colour),
                colour_field(src, ahead_column, colour),
                ahead_columns,
            )
            behind = zip_colour(
                colour_field(carried, here, colour),
                colour_field(carried, behind_column, colour),
                behind_columns,
            )
            return add_colour(times(link, ahead), behind)

        def x_part(links, src, colour):
            link = load_link(links, base, 1, 0)
            value = colour_field(src, here, colour)
            ahead = times(link, map_colour(value, x_ahead))
            return add_colour(ahead, map_colour(times_adjoint(link, value), x_behind))

        def y_parts(colour):
            link_a = load_link(links_a, base, 1, 1)
            value_a = colour_field(src_a, here, colour)
            product_a = times_adjoint(link_a, value_a)
            if rims == 0:
                ahead_a = times(link_a, map_colour(value_a, lambda v: roll(v, -1, 0)))
                return [add_colour(ahead_a, map_colour(product_a, lambda v: roll(v, 1, 0)))]
            link_b = load_link(links_b, base, 1, 1)
            value_b = colour_field(src_b, here, colour)
            product_b = times_adjoint(link_b, value_b)
            parts = [
                add_colour(
                    times(link_a, zip_colour(value_a, value_b, ahead_rows)),
                    zip_colour(product_a, product_b, behind_rows),
                )
            ]
            if rims == 2:
                parts.append(
                    add_colour(
                        times(link_b, zip_colour(value_b, value_a, ahead_rows)),
                        zip_colour(product_b, product_a, behind_rows),
                    )
                )
            return parts

        for colour in range(3):
            jobs = [(links_a, src_a, carried_a, dst_a), (links_b, src_b, carried_b, dst_b)]
            for (links, src, carried, dst), y_part in zip(jobs, y_parts(colour)):
                total = add_colour(x_part(links, src, colour), y_part)
                total = add_colour(total, z_part(links, src, carried, colour))
                store_colour(
                    dst, here, colour, next_field(colour_field(src, here, colour), total)
                )
        return carry

    lax.fori_loop(0, updates[0], update, 0)


def smear_first_kernel(
    own, own_p, below, below_p, above, above_p, links_a, links_b, out,
    mask_a, mask_b, fa, fb, ga, gb, ca, cb,
):
    low = rows() < 4
    even = lax.axis_index("gc") == 0

    def build(block, carry):
        for mine, down, up, column in (
            (own, below, above, 2 * block),
            (own_p, below_p, above_p, jnp.where(even, 2 * block + 1, 3 - 2 * block)),
        ):
            for k in range(28):
                start = pl.multiple_of(block * 224 + 8 * k, 8)
                tiles = gather_rows(
                    mine[pl.ds(start, 8)], down[pl.ds(start, 8)], up[pl.ds(start, 8)]
                )
                if k < 27:
                    for odd in range(2):
                        links_a[column * 54 + 2 * k + odd] = tiles[odd][0]
                        links_b[column * 54 + 2 * k + odd] = tiles[odd][1]
            mask_a[column], mask_b[column] = tiles[0]
        return carry

    lax.fori_loop(0, 2, build, 0)
    every, near = (4, four_columns), (3, nearest)
    point_iteration(links_a, links_b, mask_a, mask_b, ga, gb)
    smear_iteration(links_a, links_b, ga, gb, fa, fb, ca, cb, 1, every, every)
    smear_iteration(links_a, links_b, fa, fb, ga, gb, ca, cb, 0, every, every)
    smear_iteration(links_a, links_b, ga, gb, fa, fb, ca, cb, 0, every, near)

    def pack(i, carry):
        column = nearest(i)
        for k in range(9):
            even = roll(fa[column * 18 + 2 * k], 6, 0)
            odd = roll(fa[column * 18 + 2 * k + 1], 2, 0)
            out[i * 9 + k] = jnp.where(low, even, odd)
        return carry

    lax.fori_loop(0, 3, pack, 0)


def smear_second_kernel(links_a, links_b, own, below, above, out, fa, fb, ga, gb, ca, cb):
    low = rows() < 4

    def build(i, carry):
        column = nearest(i)
        for k in range(9):
            index = i * 9 + k
            tiles = gather_rows(own[index], below[index], above[index])
            for odd in range(2):
                fa[column * 18 + 2 * k + odd] = tiles[odd][0]
                fb[column * 18 + 2 * k + odd] = tiles[odd][1]
        return carry

    lax.fori_loop(0, 3, build, 0)
    near, pair, one = (3, nearest), (2, lambda i: 3 * i), (1, four_columns)
    smear_iteration(links_a, links_b, fa, fb, ga, gb, ca, cb, 2, near, near)
    smear_iteration(links_a, links_b, ga, gb, fa, fb, ca, cb, 1, near, near)
    smear_iteration(links_a, links_b, fa, fb, ga, gb, ca, cb, 0, near, near)
    smear_iteration(links_a, links_b, ga, gb, fa, fb, ca, cb, 0, pair, one)
    for i in range(18):
        out[i] = jnp.where(low, roll(fa[i], 6, 0), roll(fa[i], 2, 0))


def call(kernel, outs, args, scratch=(), flops=0):
    vmem = pl.BlockSpec(memory_space=pltpu.VMEM)
    return pl.pallas_call(
        kernel,
        out_shape=[jax.ShapeDtypeStruct(shape, jnp.float32) for shape in outs],
        in_specs=[vmem] * len(args),
        out_specs=[vmem] * len(outs),
        scratch_shapes=[pltpu.VMEM(shape, jnp.float32) for shape in scratch],
        compiler_params=pltpu.CompilerParams(vmem_limit_bytes=12 << 20),
        cost_estimate=pl.CostEstimate(flops=flops, bytes_accessed=0, transcendentals=0),
    )(*args)


def shift(value, axis, amount):
    n = lax.axis_size(axis)
    return lax.ppermute(value, axis, [(i, (i + amount) % n) for i in range(n)])


FULL = (144, 8, 128)
HALF = (72, 8, 128)
RIM = (18, 8, 128)
SENDS = [HALF, HALF, RIM, RIM, RIM, RIM, HALF, HALF]


def swap(value, axis, offset=0):
    n = lax.axis_size(axis)
    pairs = [((i + offset) % n, (i + 1 + offset) % n) for i in range(0, n, 2)]
    return lax.ppermute(value, axis, pairs + [(j, i) for i, j in pairs])


def exchange(sends):
    ta, tb, ya, yb, zp, zo, *carried = sends
    times = (shift(ta, "ta", -1), shift(tb, "ta", 1))
    spaces = (shift(ya, "xy", -1), shift(yb, "xy", 1), swap(zp, "gc"), swap(zo, GZ, 1))
    return (*times, *spaces, *carried)


def whole_step(links, guess, source_sites):
    n_time = lax.axis_size("ta")
    reduced = ("ta", "gh", "xy")
    link_rows = links.reshape(288, 128)
    guess_rows = guess.reshape(1152, 128)

    block = pl.pallas_call(
        block_kernel,
        name="block",
        out_shape=jax.ShapeDtypeStruct((224, 128), jnp.float32),
        in_specs=[pl.BlockSpec(memory_space=pltpu.MemorySpace.HBM)] * 2,
        out_specs=pl.BlockSpec(memory_space=pltpu.VMEM),
        scratch_shapes=[pltpu.SMEM((1, 4), jnp.int32)] + [pltpu.SemaphoreType.DMA] * 2,
        compiler_params=pltpu.CompilerParams(vmem_limit_bytes=12 << 20),
    )(source_sites.reshape(1, 4), link_rows)
    far = swap(block, "gh")
    (own,) = call(columns_kernel, [(448, 128)], (block, far))
    below, above = shift(own, "xy", 1), shift(own, "xy", -1)
    own_p = swap(own, "gc")
    below_p, above_p = swap(below, "gc"), swap(above, "gc")

    def prepare(*refs):
        prepare_kernel(n_time - 1, *refs)

    field, pair_links, *sends = call(
        prepare, [FULL, HALF] + SENDS, (guess_rows, link_rows), flops=4000000
    )
    halos = exchange(sends)
    (applied,) = call(first_kernel, [FULL], (field, pair_links, *halos), flops=8000000)

    tiles = [(72, 8, 128)] * 6
    links_a, links_b, smeared = call(
        smear_first_kernel,
        [(216, 8, 128), (216, 8, 128), (27, 8, 128)],
        (own, own_p, below, below_p, above, above_p),
        scratch=[(4, 8, 128)] * 2 + tiles,
        flops=30000000,
    )
    below, above = shift(smeared, "xy", 1), shift(smeared, "xy", -1)
    (smeared,) = call(
        smear_second_kernel,
        [(18, 8, 128)],
        (links_a, links_b, smeared, below, above),
        scratch=tiles,
        flops=30000000,
    )
    defect, *sends = call(
        defect_kernel, [FULL] + SENDS, (applied, smeared, pair_links), flops=4000000
    )
    search, norm, *sends = call(
        search_kernel,
        [FULL, (8, 128)] + SENDS,
        (defect, pair_links, *exchange(sends)),
        scratch=[(PAIRS, 8, 128)],
        flops=12000000,
    )
    applied, sums = call(
        applied_kernel,
        [FULL, (8, 128)],
        (search, pair_links, *exchange(sends), norm),
        scratch=[(PAIRS, 8, 128)],
        flops=12000000,
    )
    partner = swap(sums, "gc")
    (sums,) = call(middle_kernel, [(lax.axis_size(reduced), 128)], (sums, partner))
    sums = lax.all_to_all(sums, reduced, 0, 0, tiled=True)
    sends = call(last_sends_kernel, SENDS[:6], (applied, pair_links), flops=4000000)
    halos = exchange(sends)
    (normal,) = call(stencil_kernel, [FULL], (applied, pair_links, *halos), flops=8000000)
    solution, residual = call(
        final_kernel,
        [(1152, 128), (1152, 128)],
        (normal, sums, guess_rows, search),
        scratch=[(PAIRS, 8, 128)],
        flops=2000000,
    )
    return solution.reshape(guess.shape), residual.reshape(guess.shape)


def solution(mesh):
    n_time, n_z, n_y = (mesh.shape[axis] for axis in ("ta", "gz", "xy"))
    finer = Mesh(mesh.devices.reshape(n_time, n_z // 2, 2, n_y), ("ta", "gh", "gc", "xy"))
    spec = P(None, None, None, None, "ta", "xy", GZ)
    return jax.shard_map(
        whole_step,
        mesh=finer,
        in_specs=(spec, spec, P("ta", "xy", GZ, None)),
        out_specs=(spec, spec),
        check_vma=False,
    )
```

```python
import jax
import jax.numpy as jnp
import numpy as np
from jax import lax
from jax.experimental import pallas as pl
from jax.experimental.pallas import tpu as pltpu
from jax.sharding import Mesh
from jax.sharding import PartitionSpec as P

LX = 32
HOPPING = 0.12
PAIRS = 6
GZ = ("gh", "gc")


def pauli_blocks():
    sigma_one = np.array([[0, 1], [1, 0]], dtype=complex)
    sigma_two = np.array([[0, -1j], [1j, 0]], dtype=complex)
    sigma_three = np.array([[1, 0], [0, -1]], dtype=complex)
    return [-1j * sigma_one, -1j * sigma_two, -1j * sigma_three, np.eye(2, dtype=complex)]


E_BLOCKS = pauli_blocks()


def roll(value, shift, axis):
    size = value.shape[axis]
    shift = shift % size
    return value if shift == 0 else pltpu.roll(value, shift, axis)


def rows():
    return lax.broadcasted_iota(jnp.int32, (8, 128), 0)


def lanes():
    return lax.broadcasted_iota(jnp.int32, (8, 128), 1)


def add_phase(base, phase, value):
    real, imag = value
    if phase == 1:
        return (base[0] + real, base[1] + imag)
    if phase == -1:
        return (base[0] - real, base[1] - imag)
    if phase == 1j:
        return (base[0] - imag, base[1] + real)
    return (base[0] + imag, base[1] - real)


def load_field(ref, pair):
    base = pair * 24
    return [
        [(ref[base + s * 3 + c], ref[base + 12 + s * 3 + c]) for c in range(3)] for s in range(4)
    ]


def project(field, mu, parity):
    block = E_BLOCKS[mu]
    half = []
    for a in range(2):
        b = int(np.flatnonzero(np.abs(block[a]) > 0.5)[0])
        phase = complex(parity * block[a, b])
        half.append([add_phase(field[a][c], phase, field[2 + b][c]) for c in range(3)])
    return half


def lift(total, half, mu, parity):
    block = E_BLOCKS[mu]
    for a in range(2):
        b = int(np.flatnonzero(np.abs(block[a]) > 0.5)[0])
        phase = complex(parity * np.conj(block[a, b]))
        for c in range(3):
            total[a][c] = add_phase(total[a][c], 1, half[a][c])
            total[2 + b][c] = add_phase(total[2 + b][c], phase, half[a][c])


def load_link(ref, base, stride, mu):
    return [
        [
            (
                ref[base + stride * (mu * 18 + a * 3 + b)],
                ref[base + stride * (mu * 18 + 9 + a * 3 + b)],
            )
            for b in range(3)
        ]
        for a in range(3)
    ]


def times(link, vector):
    out = []
    for a in range(3):
        real = imag = None
        for b in range(3):
            ur, ui = link[a][b]
            vr, vi = vector[b]
            tr = ur * vr - ui * vi
            ti = ur * vi + ui * vr
            real = tr if real is None else real + tr
            imag = ti if imag is None else imag + ti
        out.append((real, imag))
    return out


def times_adjoint(link, vector):
    out = []
    for a in range(3):
        real = imag = None
        for b in range(3):
            ur, ui = link[b][a]
            vr, vi = vector[b]
            tr = ur * vr + ui * vi
            ti = ur * vi - ui * vr
            real = tr if real is None else real + tr
            imag = ti if imag is None else imag + ti
        out.append((real, imag))
    return out


def flat(half):
    return [half[a][c][part] for part in range(2) for a in range(2) for c in range(3)]


def unflat(values):
    return [[(values[a * 3 + c], values[6 + a * 3 + c]) for c in range(3)] for a in range(2)]


def map_half(half, fn):
    return [[(fn(re), fn(im)) for re, im in spin] for spin in half]


def pick4(index, parts):
    return jnp.where(
        index < 2,
        jnp.where(index == 0, parts[0], parts[1]),
        jnp.where(index == 2, parts[2], parts[3]),
    )


def x_ahead(value):
    return jnp.where(lanes() % LX == LX - 1, roll(value, LX - 1, 1), roll(value, -1, 1))


def x_behind(value):
    return jnp.where(lanes() % LX == 0, roll(value, 1 - LX, 1), roll(value, 1, 1))


def make_sends(field, pair, links, sign, outs):
    t_ahead, t_behind, y_ahead, y_behind, z_partner, z_other, *carried = outs
    even = lax.axis_index("gc") == 0
    row4 = rows() % 4
    group = lanes() // LX
    half = flat(project(field, 3, -sign))
    for i in range(12):
        t_ahead[pair * 12 + i] = half[i]
    link = load_link(links, 0, 1, 3)
    half = flat([times_adjoint(link, v) for v in project(field, 3, sign)])
    for i in range(12):
        t_behind[pair * 12 + i] = half[i]
    half = flat(project(field, 1, -sign))
    for q in range(3):
        y_ahead[pair * 3 + q] = pick4(row4, [roll(half[4 * q + j], j, 0) for j in range(4)])
    link = load_link(links, 0, 1, 1)
    half = flat([times_adjoint(link, v) for v in project(field, 1, sign)])
    for i in range(12 if carried else 0):
        carried[0][pair * 12 + i] = half[i]
    for q in range(3):
        y_behind[pair * 3 + q] = pick4(row4, [roll(half[4 * q + j], j - 3, 0) for j in range(4)])
    half = flat(project(field, 2, -sign))
    first = [pick4(group, [roll(half[4 * q + j], LX * j, 1) for j in range(4)]) for q in range(3)]
    link = load_link(links, 0, 1, 2)
    half = flat([times_adjoint(link, v) for v in project(field, 2, sign)])
    for i in range(12 if carried else 0):
        carried[1][pair * 12 + i] = half[i]
    for q in range(3):
        last = pick4(group, [roll(half[4 * q + j], LX * (j - 3), 1) for j in range(4)])
        z_partner[pair * 3 + q] = jnp.where(even, last, first[q])
        z_other[pair * 3 + q] = jnp.where(even, first[q], last)


def apply_wilson(field, pair, links, sign, halos, *carried):
    t_ahead, t_behind, y_ahead, y_behind, z_partner, z_other = halos
    even = lax.axis_index("gc") == 0
    row4 = rows() % 4
    group = lanes() // LX

    def carried_tiles(mu):
        if carried:
            return [carried[mu - 1][pair * 12 + i] for i in range(12)]
        return flat([times_adjoint(link, v) for v in project(field, mu, sign)])

    zero = jnp.zeros((8, 128), jnp.float32)
    total = [[(zero, zero) for _ in range(3)] for _ in range(4)]
    link = load_link(links, 0, 1, 0)
    half = map_half(project(field, 0, -sign), x_ahead)
    lift(total, [times(link, v) for v in half], 0, -sign)
    half = [times_adjoint(link, v) for v in project(field, 0, sign)]
    lift(total, map_half(half, x_behind), 0, sign)
    link = load_link(links, 0, 1, 1)
    half = flat(project(field, 1, -sign))
    packed = [y_ahead[pair * 3 + q] for q in range(3)]
    half = [
        jnp.where(row4 == 3, roll(packed[i // 4], 3 - i % 4, 0), roll(half[i], -1, 0))
        for i in range(12)
    ]
    lift(total, [times(link, v) for v in unflat(half)], 1, -sign)
    packed = [y_behind[pair * 3 + q] for q in range(3)]
    own = carried_tiles(1)
    half = [
        jnp.where(row4 == 0, roll(packed[i // 4], -(i % 4), 0), roll(own[i], 1, 0))
        for i in range(12)
    ]
    lift(total, unflat(half), 1, sign)
    link = load_link(links, 0, 1, 2)
    half = flat(project(field, 2, -sign))
    packed = [
        jnp.where(even, z_partner[pair * 3 + q], z_other[pair * 3 + q]) for q in range(3)
    ]
    half = [
        jnp.where(group == 3, roll(packed[i // 4], LX * (3 - i % 4), 1), roll(half[i], -LX, 1))
        for i in range(12)
    ]
    lift(total, [times(link, v) for v in unflat(half)], 2, -sign)
    packed = [
        jnp.where(even, z_other[pair * 3 + q], z_partner[pair * 3 + q]) for q in range(3)
    ]
    own = carried_tiles(2)
    half = [
        jnp.where(group == 0, roll(packed[i // 4], -LX * (i % 4), 1), roll(own[i], LX, 1))
        for i in range(12)
    ]
    lift(total, unflat(half), 2, sign)
    link = load_link(links, 0, 1, 3)
    half = unflat([t_ahead[pair * 12 + i] for i in range(12)])
    lift(total, [times(link, v) for v in half], 3, -sign)
    half = unflat([t_behind[pair * 12 + i] for i in range(12)])
    lift(total, half, 3, sign)
    return [
        [
            tuple(field[s][c][k] - HOPPING * total[s][c][k] for k in range(2))
            for c in range(3)
        ]
        for s in range(4)
    ]


def store_field(ref, pair, field):
    for s in range(4):
        for c in range(3):
            ref[pair * 24 + s * 3 + c] = field[s][c][0]
            ref[pair * 24 + 12 + s * 3 + c] = field[s][c][1]


def norm_row(partials, offset):
    row = rows()
    lane = lanes()
    total = jnp.zeros((8, 128), jnp.float32)
    for pair in range(PAIRS):
        sums = jnp.sum(partials[pair], axis=1, keepdims=True)
        keep = lane == offset + 2 * pair + row // 4
        total = total + jnp.where(keep, sums, 0.0)
    return jnp.sum(total, axis=0, keepdims=True)


def squares(field):
    total = None
    for s in range(4):
        for c in range(3):
            for k in range(2):
                term = field[s][c][k] * field[s][c][k]
                total = term if total is None else total + term
    return total


def block_kernel(source, links, out, sites, link_done, site_done):
    link_copy = pltpu.make_async_copy(links.at[0:216], out.at[0:216], link_done)
    site_copy = pltpu.make_async_copy(source, sites, site_done)
    link_copy.start()
    site_copy.start()
    site_copy.wait()
    hit = (rows() == sites[0, 1]) & (lanes() == sites[0, 2] * LX + sites[0, 3]) & (sites[0, 0] == 0)
    out[216:224] = jnp.where(hit, 1.0, 0.0).astype(jnp.float32)
    link_copy.wait()


def prepare_kernel(last_time, guess, links, field, pair_links, *sends):
    low = rows() < 4
    for k in range(36):
        value = links[8 * k : 8 * k + 8]
        if k >= 27:
            crossing = lax.axis_index("ta") == last_time
            value = jnp.where(crossing, -value, value)
        other = roll(value, 4, 0)
        pair_links[2 * k] = jnp.where(low, value, other)
        pair_links[2 * k + 1] = jnp.where(low, other, value)

    def body(pair, carry):
        for k in range(12):
            start = pl.multiple_of(pair * 192 + 8 * k, 8)
            first = guess[pl.ds(start, 8)]
            second = guess[pl.ds(start + 96, 8)]
            field[pair * 24 + 2 * k] = jnp.where(low, first, roll(second, 4, 0))
            field[pair * 24 + 2 * k + 1] = jnp.where(low, roll(first, 4, 0), second)
        make_sends(load_field(field, pair), pair, pair_links, 1.0, sends)
        return carry

    lax.fori_loop(0, PAIRS, body, 0)


def first_kernel(field, links, ta, tb, ya, yb, za, zb, cy, cz, out):
    def body(pair, carry):
        value = apply_wilson(
            load_field(field, pair), pair, links, 1.0, (ta, tb, ya, yb, za, zb), cy, cz
        )
        store_field(out, pair, value)
        return carry

    lax.fori_loop(0, PAIRS, body, 0)


def defect_kernel(applied, smeared, links, out, *sends):
    low = rows() < 4
    for pair in range(PAIRS):
        spins = [(2 * pair + h) // 3 for h in range(2)]
        colours = [(2 * pair + h) % 3 for h in range(2)]
        for part in range(2):
            for s in range(4):
                for a in range(3):
                    index = pair * 24 + part * 12 + s * 3 + a
                    source = [
                        smeared[colours[h] * 6 + part * 3 + a] if spins[h] == s else 0.0
                        for h in range(2)
                    ]
                    if s in spins:
                        out[index] = jnp.where(low, source[0], source[1]) - applied[index]
                    else:
                        out[index] = -applied[index]

    def body(pair, carry):
        make_sends(load_field(out, pair), pair, links, -1.0, sends)
        return carry

    lax.fori_loop(0, PAIRS, body, 0)


def search_kernel(field, links, ta, tb, ya, yb, za, zb, cy, cz, out, norm, *rest):
    sends, partials = rest[:8], rest[8]

    def body(pair, carry):
        value = apply_wilson(
            load_field(field, pair), pair, links, -1.0, (ta, tb, ya, yb, za, zb), cy, cz
        )
        store_field(out, pair, value)
        partials[pair] = squares(value)
        make_sends(load_field(out, pair), pair, links, 1.0, sends)
        return carry

    lax.fori_loop(0, PAIRS, body, 0)
    norm[...] = jnp.broadcast_to(norm_row([partials[p] for p in range(PAIRS)], 0), (8, 128))


def applied_kernel(field, links, ta, tb, ya, yb, za, zb, cy, cz, norm, out, sums, partials):
    def body(pair, carry):
        value = apply_wilson(
            load_field(field, pair), pair, links, 1.0, (ta, tb, ya, yb, za, zb), cy, cz
        )
        store_field(out, pair, value)
        partials[pair] = squares(value)
        return carry

    lax.fori_loop(0, PAIRS, body, 0)
    row = norm_row([partials[p] for p in range(PAIRS)], 16)
    sums[...] = norm[...] + jnp.broadcast_to(row, (8, 128))


def last_sends_kernel(field, links, *sends):
    def body(pair, carry):
        make_sends(load_field(field, pair), pair, links, -1.0, sends)
        return carry

    lax.fori_loop(0, PAIRS, body, 0)


def stencil_kernel(field, links, ta, tb, ya, yb, za, zb, out):
    def body(pair, carry):
        value = apply_wilson(
            load_field(field, pair), pair, links, -1.0, (ta, tb, ya, yb, za, zb)
        )
        store_field(out, pair, value)
        return carry

    lax.fori_loop(0, PAIRS, body, 0)


def column_sums(ref):
    parts = [ref[8 * k : 8 * k + 8] for k in range(ref.shape[0] // 8)]
    while len(parts) > 1:
        odd = parts[-1:] if len(parts) % 2 else []
        parts = [a + b for a, b in zip(parts[::2], parts[1::2])] + odd
    return jnp.broadcast_to(jnp.sum(parts[0], axis=0, keepdims=True), (8, 128))


def middle_kernel(own, partner, out):
    total = own[...] + partner[...]
    for k in range(out.shape[0] // 8):
        out[8 * k : 8 * k + 8] = total


def column_kernel(sums, out):
    out[...] = column_sums(sums)


def columns_kernel(own, far, out):
    out[0:224] = own[...]
    out[224:448] = far[...]


def final_kernel(
    normal, sums, sums_far, guess, search, solution, residual, steps, new_solution, new_residual, done
):
    low = rows() < 4
    lane = lanes()
    total = sums[...] + sums_far[...]
    curvature = jnp.where(lane < 12, roll(total, -16, 1), 1.0)
    ratio = total / curvature
    for pair in range(PAIRS):
        keep = lane == 2 * pair + rows() // 4
        step = jnp.sum(jnp.where(keep, ratio, 0.0), axis=1, keepdims=True)
        steps[pair] = jnp.broadcast_to(step, (8, 128))

    def copies(pair):
        span = pl.ds(pl.multiple_of(pair * 192, 8), 192)
        return (
            pltpu.make_async_copy(new_solution.at[span], solution.at[span], done.at[0, pair]),
            pltpu.make_async_copy(new_residual.at[span], residual.at[span], done.at[1, pair]),
        )

    def body(pair, carry):
        step = steps[pair]
        for k in range(12):
            index = pair * 24 + 2 * k
            start = pl.multiple_of(pair * 192 + 8 * k, 8)
            even, odd = search[index], search[index + 1]
            left = even - step * normal[index], odd - step * normal[index + 1]
            even, odd = step * even, step * odd
            new_residual[pl.ds(start, 8)] = jnp.where(low, left[0], roll(left[1], 4, 0))
            new_residual[pl.ds(start + 96, 8)] = jnp.where(low, roll(left[0], 4, 0), left[1])
            new_solution[pl.ds(start, 8)] = guess[pl.ds(start, 8)] + jnp.where(
                low, even, roll(odd, 4, 0)
            )
            new_solution[pl.ds(start + 96, 8)] = guess[pl.ds(start + 96, 8)] + jnp.where(
                low, roll(even, 4, 0), odd
            )
        for copy in copies(pair):
            copy.start()
        return carry

    lax.fori_loop(0, PAIRS, body, 0)
    for pair in range(PAIRS):
        for copy in copies(pair):
            copy.wait()


def gather_rows(own, below, above):
    row = rows()
    inside = (row >= 2) & (row < 6)
    out = []
    for odd in range(2):
        shift = 6 if odd else 2
        o = roll(own, shift, 0)
        lo = roll(below, 8 - shift, 0)
        hi = roll(above, 8 - shift, 0)
        tile_a = jnp.where(inside, o, jnp.where(row < 2, lo, hi))
        tile_b = jnp.where(row < 4, hi, lo)
        out.append((tile_a, tile_b))
    return out


def colour_field(ref, base, colour):
    return [(ref[base + colour * 6 + a], ref[base + colour * 6 + 3 + a]) for a in range(3)]


def store_colour(ref, base, colour, value):
    for a in range(3):
        ref[base + colour * 6 + a] = value[a][0]
        ref[base + colour * 6 + 3 + a] = value[a][1]


def map_colour(value, fn):
    return [(fn(re), fn(im)) for re, im in value]


def zip_colour(first, second, fn):
    return [(fn(a[0], b[0]), fn(a[1], b[1])) for a, b in zip(first, second)]


def nearest(i):
    return i + (i >> 1)


def four_columns(i):
    return i


def ahead_rows(first, second):
    return jnp.where(rows() == 7, roll(second, -1, 0), roll(first, -1, 0))


def behind_rows(first, second):
    return jnp.where(rows() == 0, roll(second, 1, 0), roll(first, 1, 0))


def ahead_columns(first, second):
    return jnp.where(lanes() < 96, roll(first, -LX, 1), roll(second, -LX, 1))


def behind_columns(first, second):
    return jnp.where(lanes() >= LX, roll(first, LX, 1), roll(second, LX, 1))


def add_colour(first, second):
    return zip_colour(first, second, lambda a, b: a + b)


def next_field(value, total):
    return zip_colour(value, total, lambda a, b: (a + 0.25 * b) * 0.5)


def point_iteration(links_a, links_b, mask_a, mask_b, dst_a, dst_b):
    def update(column, carry):
        base = column * 54
        behind_column = (column + 3) & 3
        ahead_column = (column + 1) & 3
        here_a, here_b = mask_a[column], mask_b[column]

        def conjugate(links, where, mu, colour, mask):
            link = load_link(links, where * 54, 1, mu)
            return [(link[colour][a][0] * mask, -link[colour][a][1] * mask) for a in range(3)]

        for links, dst, mask, other_mask, others in (
            (links_a, dst_a, here_a, here_b, links_b),
            (links_b, dst_b, here_b, here_a, links_a),
        ):
            masks = mask_a if dst is dst_a else mask_b
            shifted = [
                x_ahead(mask),
                ahead_rows(mask, other_mask),
                ahead_columns(mask, masks[ahead_column]),
            ]
            for colour in range(3):
                total = [
                    (shifted[0] * re, shifted[0] * im)
                    for re, im in (row[colour] for row in load_link(links, base, 1, 0))
                ]
                for mu in (1, 2):
                    link = load_link(links, base, 1, mu)
                    total = add_colour(
                        total,
                        [(shifted[mu] * r[colour][0], shifted[mu] * r[colour][1]) for r in link],
                    )
                product = conjugate(links, column, 0, colour, mask)
                total = add_colour(total, map_colour(product, x_behind))
                product = conjugate(links, column, 1, colour, mask)
                other = conjugate(others, column, 1, colour, other_mask)
                total = add_colour(total, zip_colour(product, other, behind_rows))
                product = conjugate(links, column, 2, colour, mask)
                other = conjugate(links, behind_column, 2, colour, masks[behind_column])
                total = add_colour(total, zip_colour(product, other, behind_columns))
                zero = jnp.zeros((8, 128), jnp.float32)
                value = [(mask if a == colour else zero, zero) for a in range(3)]
                store_colour(dst, column * 18, colour, next_field(value, total))
        return carry

    lax.fori_loop(0, 4, update, 0)


def smear_iteration(
    links_a, links_b, src_a, src_b, dst_a, dst_b, carried_a, carried_b, rims, carries, updates
):
    def carry_z(i, carry):
        column = carries[1](i)
        jobs = [(links_a, src_a, carried_a)] + [(links_b, src_b, carried_b)] * (rims == 2)
        for links, src, carried in jobs:
            link = load_link(links, column * 54, 1, 2)
            for colour in range(3):
                value = times_adjoint(link, colour_field(src, column * 18, colour))
                store_colour(carried, column * 18, colour, value)
        return carry

    lax.fori_loop(0, carries[0], carry_z, 0)

    def update(i, carry):
        column = updates[1](i)
        base = column * 54
        here = column * 18
        ahead_column = ((column + 1) & 3) * 18
        behind_column = ((column + 3) & 3) * 18

        def z_part(links, src, carried, colour):
            link = load_link(links, base, 1, 2)
            ahead = zip_colour(
                colour_field(src, here, colour),
                colour_field(src, ahead_column, colour),
                ahead_columns,
            )
            behind = zip_colour(
                colour_field(carried, here, colour),
                colour_field(carried, behind_column, colour),
                behind_columns,
            )
            return add_colour(times(link, ahead), behind)

        def x_part(links, src, colour):
            link = load_link(links, base, 1, 0)
            value = colour_field(src, here, colour)
            ahead = times(link, map_colour(value, x_ahead))
            return add_colour(ahead, map_colour(times_adjoint(link, value), x_behind))

        def y_parts(colour):
            link_a = load_link(links_a, base, 1, 1)
            value_a = colour_field(src_a, here, colour)
            product_a = times_adjoint(link_a, value_a)
            if rims == 0:
                ahead_a = times(link_a, map_colour(value_a, lambda v: roll(v, -1, 0)))
                return [add_colour(ahead_a, map_colour(product_a, lambda v: roll(v, 1, 0)))]
            link_b = load_link(links_b, base, 1, 1)
            value_b = colour_field(src_b, here, colour)
            product_b = times_adjoint(link_b, value_b)
            parts = [
                add_colour(
                    times(link_a, zip_colour(value_a, value_b, ahead_rows)),
                    zip_colour(product_a, product_b, behind_rows),
                )
            ]
            if rims == 2:
                parts.append(
                    add_colour(
                        times(link_b, zip_colour(value_b, value_a, ahead_rows)),
                        zip_colour(product_b, product_a, behind_rows),
                    )
                )
            return parts

        for colour in range(3):
            jobs = [(links_a, src_a, carried_a, dst_a), (links_b, src_b, carried_b, dst_b)]
            for (links, src, carried, dst), y_part in zip(jobs, y_parts(colour)):
                total = add_colour(x_part(links, src, colour), y_part)
                total = add_colour(total, z_part(links, src, carried, colour))
                store_colour(
                    dst, here, colour, next_field(colour_field(src, here, colour), total)
                )
        return carry

    lax.fori_loop(0, updates[0], update, 0)


def smear_first_kernel(
    own, own_p, below, below_p, above, above_p, links_a, links_b, out,
    mask_a, mask_b, fa, fb, ga, gb, ca, cb,
):
    low = rows() < 4
    even = lax.axis_index("gc") == 0

    def build(block, carry):
        for mine, down, up, column in (
            (own, below, above, 2 * block),
            (own_p, below_p, above_p, jnp.where(even, 2 * block + 1, 3 - 2 * block)),
        ):
            for k in range(28):
                start = pl.multiple_of(block * 224 + 8 * k, 8)
                tiles = gather_rows(
                    mine[pl.ds(start, 8)], down[pl.ds(start, 8)], up[pl.ds(start, 8)]
                )
                if k < 27:
                    for odd in range(2):
                        links_a[column * 54 + 2 * k + odd] = tiles[odd][0]
                        links_b[column * 54 + 2 * k + odd] = tiles[odd][1]
            mask_a[column], mask_b[column] = tiles[0]
        return carry

    lax.fori_loop(0, 2, build, 0)
    every, near = (4, four_columns), (3, nearest)
    point_iteration(links_a, links_b, mask_a, mask_b, ga, gb)
    smear_iteration(links_a, links_b, ga, gb, fa, fb, ca, cb, 1, every, every)
    smear_iteration(links_a, links_b, fa, fb, ga, gb, ca, cb, 0, every, every)
    smear_iteration(links_a, links_b, ga, gb, fa, fb, ca, cb, 0, every, near)

    def pack(i, carry):
        column = nearest(i)
        for k in range(9):
            even = roll(fa[column * 18 + 2 * k], 6, 0)
            odd = roll(fa[column * 18 + 2 * k + 1], 2, 0)
            out[i * 9 + k] = jnp.where(low, even, odd)
        return carry

    lax.fori_loop(0, 3, pack, 0)


def smear_second_kernel(links_a, links_b, own, below, above, out, fa, fb, ga, gb, ca, cb):
    low = rows() < 4

    def build(i, carry):
        column = nearest(i)
        for k in range(9):
            index = i * 9 + k
            tiles = gather_rows(own[index], below[index], above[index])
            for odd in range(2):
                fa[column * 18 + 2 * k + odd] = tiles[odd][0]
                fb[column * 18 + 2 * k + odd] = tiles[odd][1]
        return carry

    lax.fori_loop(0, 3, build, 0)
    near, pair, one = (3, nearest), (2, lambda i: 3 * i), (1, four_columns)
    smear_iteration(links_a, links_b, fa, fb, ga, gb, ca, cb, 2, near, near)
    smear_iteration(links_a, links_b, ga, gb, fa, fb, ca, cb, 1, near, near)
    smear_iteration(links_a, links_b, fa, fb, ga, gb, ca, cb, 0, near, near)
    smear_iteration(links_a, links_b, ga, gb, fa, fb, ca, cb, 0, pair, one)
    for i in range(18):
        out[i] = jnp.where(low, roll(fa[i], 6, 0), roll(fa[i], 2, 0))


def call(kernel, outs, args, scratch=(), flops=0):
    vmem = pl.BlockSpec(memory_space=pltpu.VMEM)
    return pl.pallas_call(
        kernel,
        out_shape=[jax.ShapeDtypeStruct(shape, jnp.float32) for shape in outs],
        in_specs=[vmem] * len(args),
        out_specs=[vmem] * len(outs),
        scratch_shapes=[pltpu.VMEM(shape, jnp.float32) for shape in scratch],
        compiler_params=pltpu.CompilerParams(vmem_limit_bytes=12 << 20),
        cost_estimate=pl.CostEstimate(flops=flops, bytes_accessed=0, transcendentals=0),
    )(*args)


def shift(value, axis, amount):
    n = lax.axis_size(axis)
    return lax.ppermute(value, axis, [(i, (i + amount) % n) for i in range(n)])


FULL = (144, 8, 128)
HALF = (72, 8, 128)
RIM = (18, 8, 128)
SENDS = [HALF, HALF, RIM, RIM, RIM, RIM, HALF, HALF]


def swap(value, axis, offset=0):
    n = lax.axis_size(axis)
    pairs = [((i + offset) % n, (i + 1 + offset) % n) for i in range(0, n, 2)]
    return lax.ppermute(value, axis, pairs + [(j, i) for i, j in pairs])


def exchange(sends):
    ta, tb, ya, yb, zp, zo, *carried = sends
    spaces = (shift(ya, "xy", -1), shift(yb, "xy", 1), swap(zp, "gc"), swap(zo, GZ, 1))
    times = (shift(ta, "ta", -1), shift(tb, "ta", 1))
    return (*times, *spaces, *carried)


def whole_step(links, guess, source_sites):
    n_time = lax.axis_size("ta")
    reduced = ("ta", "xy")
    link_rows = links.reshape(288, 128)
    guess_rows = guess.reshape(1152, 128)

    block = pl.pallas_call(
        block_kernel,
        name="block",
        out_shape=jax.ShapeDtypeStruct((224, 128), jnp.float32),
        in_specs=[pl.BlockSpec(memory_space=pltpu.MemorySpace.HBM)] * 2,
        out_specs=pl.BlockSpec(memory_space=pltpu.VMEM),
        scratch_shapes=[pltpu.SMEM((1, 4), jnp.int32)] + [pltpu.SemaphoreType.DMA] * 2,
        compiler_params=pltpu.CompilerParams(vmem_limit_bytes=12 << 20),
    )(source_sites.reshape(1, 4), link_rows)
    far = swap(block, "gh")
    (own,) = call(columns_kernel, [(448, 128)], (block, far))
    below, above = shift(own, "xy", 1), shift(own, "xy", -1)
    own_p = swap(own, "gc")
    below_p, above_p = swap(below, "gc"), swap(above, "gc")

    def prepare(*refs):
        prepare_kernel(n_time - 1, *refs)

    field, pair_links, *sends = call(
        prepare, [FULL, HALF] + SENDS, (guess_rows, link_rows), flops=4000000
    )
    halos = exchange(sends)
    (applied,) = call(first_kernel, [FULL], (field, pair_links, *halos), flops=8000000)

    tiles = [(72, 8, 128)] * 6
    links_a, links_b, smeared = call(
        smear_first_kernel,
        [(216, 8, 128), (216, 8, 128), (27, 8, 128)],
        (own, own_p, below, below_p, above, above_p),
        scratch=[(4, 8, 128)] * 2 + tiles,
        flops=30000000,
    )
    below, above = shift(smeared, "xy", 1), shift(smeared, "xy", -1)
    (smeared,) = call(
        smear_second_kernel,
        [(18, 8, 128)],
        (links_a, links_b, smeared, below, above),
        scratch=tiles,
        flops=30000000,
    )
    defect, *sends = call(
        defect_kernel, [FULL] + SENDS, (applied, smeared, pair_links), flops=4000000
    )
    search, norm, *sends = call(
        search_kernel,
        [FULL, (8, 128)] + SENDS,
        (defect, pair_links, *exchange(sends)),
        scratch=[(PAIRS, 8, 128)],
        flops=12000000,
    )
    applied, sums = call(
        applied_kernel,
        [FULL, (8, 128)],
        (search, pair_links, *exchange(sends), norm),
        scratch=[(PAIRS, 8, 128)],
        flops=12000000,
    )
    partner = swap(sums, "gc")
    (sums,) = call(middle_kernel, [(lax.axis_size(reduced), 128)], (sums, partner))
    sums = lax.all_to_all(sums, reduced, 0, 0, tiled=True)
    sends = call(last_sends_kernel, SENDS[:6], (applied, pair_links), flops=4000000)
    halos = exchange(sends)
    (sums,) = call(column_kernel, [(8, 128)], (sums,))
    sums_far = swap(sums, "gh")
    (normal,) = call(stencil_kernel, [FULL], (applied, pair_links, *halos), flops=8000000)
    whole = (1152, 128)
    vmem, anywhere = (pl.BlockSpec(memory_space=space) for space in (pltpu.VMEM, pl.ANY))
    solution, residual = pl.pallas_call(
        final_kernel,
        name="final",
        out_shape=[jax.ShapeDtypeStruct(whole, jnp.float32)] * 2,
        in_specs=[vmem] * 5,
        out_specs=[anywhere] * 2,
        scratch_shapes=[pltpu.VMEM((PAIRS, 8, 128), jnp.float32)]
        + [pltpu.VMEM(whole, jnp.float32)] * 2
        + [pltpu.SemaphoreType.DMA((2, PAIRS))],
        compiler_params=pltpu.CompilerParams(vmem_limit_bytes=12 << 20),
    )(normal, sums, sums_far, guess_rows, search)
    return solution.reshape(guess.shape), residual.reshape(guess.shape)


def solution(mesh):
    n_time, n_z, n_y = (mesh.shape[axis] for axis in ("ta", "gz", "xy"))
    finer = Mesh(mesh.devices.reshape(n_time, n_z // 2, 2, n_y), ("ta", "gh", "gc", "xy"))
    spec = P(None, None, None, None, "ta", "xy", GZ)
    return jax.shard_map(
        whole_step,
        mesh=finer,
        in_specs=(spec, spec, P("ta", "xy", GZ, None)),
        out_specs=(spec, spec),
        check_vma=False,
    )
```
